16 devices in a mesh: rep: 2 (over y, z), dp: 8 (over x, core).
Axes of the slice: x: 4, y: 2, z: 1, core: 2. Of those that a mesh axis runs over, the one named last changes fastest.
The devices are a block of a 4x4x8 slice.
Arguments:
- x: bfloat16 [16, 2048, 640], P(('rep', 'dp')), parts along dimension 0
- dy: bfloat16 [16, 2048, 640], P(('rep', 'dp')), parts along dimension 0
- w_gate: bfloat16 [2, 640, 3200], replicated
- w_up: bfloat16 [2, 640, 3200], replicated
- w_down: bfloat16 [2, 3200, 640], replicated
- m_w_gate: float32 [2, 640, 3200], P(None, 'dp')
- m_w_up: float32 [2, 640, 3200], P(None, 'dp')
- m_w_down: float32 [2, 3200, 640], P(None, 'dp')
- v_w_gate: float32 [2, 640, 3200], P(None, 'dp')
- v_w_up: float32 [2, 640, 3200], P(None, 'dp')
- v_w_down: float32 [2, 3200, 640], P(None, 'dp')
Outputs:
- output 1: bfloat16 [4, 640, 3200], P('rep'), parts along dimension 0
- output 2: bfloat16 [4, 640, 3200], P('rep'), parts along dimension 0
- output 3: bfloat16 [4, 3200, 640], P('rep'), parts along dimension 0
- output 4: float32 [4, 640, 3200], P('rep', 'dp'), parts along dimension 0
- output 5: float32 [4, 640, 3200], P('rep', 'dp'), parts along dimension 0
- output 6: float32 [4, 3200, 640], P('rep', 'dp'), parts along dimension 0
- output 7: float32 [4, 640, 3200], P('rep', 'dp'), parts along dimension 0
- output 8: float32 [4, 640, 3200], P('rep', 'dp'), parts along dimension 0
- output 9: float32 [4, 3200, 640], P('rep', 'dp'), parts along dimension 0
There are 2 independent parts. The reference program is written for one: setup_inputs(seed, part) draws one part's arguments, and reference() takes and returns one part's arrays. A program takes and returns all parts, laid end to end along the dimension named above; an argument that names none is the same for every part.
All inputs are finite; a program needn't handle non-finite values.
Results may differ from the reference program's by a relative error of at most 0.022.
Values are sent between devices in bfloat16 or wider.
A program may use at most 768 MiB of HBM per device.

```python
import jax
import jax.numpy as jnp
from jax import lax

SEQUENCES = 8
TOKENS = 2048
D = 640
FF = 3200
LAYERS = 2
NAMES = ("w_gate", "w_up", "w_down")
SHAPES = {"w_gate": (LAYERS, D, FF), "w_up": (LAYERS, D, FF), "w_down": (LAYERS, FF, D)}


def bump(key, n, height):
    away = (jnp.arange(n, dtype=jnp.int32) - jax.random.randint(key, (), 0, n, jnp.int32)) % n
    return jnp.where(away < n // 8, height, 1.0)


def together(key, own, strength):
    shared = jax.random.normal(key, own.shape[1:], jnp.float32)
    return (own + strength * shared) * lax.rsqrt(1 + strength * strength)


def setup_inputs(seed: int = 0, part: int = 0) -> dict:
    kx, kdy, ka, kb, kz, kf, kh, kl, *keys = jax.random.split(jax.random.key(seed), 8 + 3 * len(NAMES))
    kx, kdy, ka, kb = (jax.random.fold_in(k, part) for k in (kx, kdy, ka, kb))
    kw, km, kv = (keys[i::3] for i in range(3))
    shape = (SEQUENCES, TOKENS, D)
    much_x, much_dy = jax.random.uniform(kz, (2,), jnp.float32, 0.0, 1.0)
    loud = 2.0 ** jax.random.uniform(jax.random.fold_in(kz, 1), (), jnp.float32, -1.0, 2.0)
    layers = 2.0 ** jax.random.uniform(kl, (LAYERS, 1, 1), jnp.float32, -1.0, 1.0)
    x = together(ka, jax.random.normal(kx, shape, jnp.float32), much_x) * bump(kf, D, 4.0)
    dy = together(kb, jax.random.normal(kdy, shape, jnp.float32), much_dy)
    drawn = {"x": x.astype(jnp.bfloat16), "dy": (loud * dy * (SEQUENCES * TOKENS) ** -0.5).astype(jnp.bfloat16)}
    for key, name in zip(kw, NAMES, strict=True):
        w = jax.random.normal(key, SHAPES[name], jnp.float32) * SHAPES[name][1] ** -0.5
        drawn[name] = (w * {"w_gate": 1.0, "w_up": bump(kh, FF, 4.0), "w_down": layers}[name]).astype(jnp.bfloat16)
    for key, name in zip(km, NAMES, strict=True):
        drawn[f"m_{name}"] = 0.1 * jax.random.normal(key, SHAPES[name], jnp.float32)
    for key, name in zip(kv, NAMES, strict=True):
        drawn[f"v_{name}"] = jax.random.uniform(key, SHAPES[name], jnp.float32, 0.005, 0.015)
    return drawn


def matmul(a, w):
    return jnp.dot(a, w, preferred_element_type=jnp.float32).astype(jnp.bfloat16)


def normed(h):
    wide = h.astype(jnp.float32)
    scale = lax.rsqrt(jnp.mean(wide**2, -1, keepdims=True) + 1e-6)
    return (wide * scale).astype(jnp.bfloat16)


def layer(h, w):
    a = normed(h)
    gate = jnp.dot(a, w["w_gate"], preferred_element_type=jnp.float32)
    up = jnp.dot(a, w["w_up"], preferred_element_type=jnp.float32)
    return h + matmul((jax.nn.silu(gate) * up).astype(jnp.bfloat16), w["w_down"])


def adamw(w, m, v, g):
    m = 0.9 * m + 0.1 * g
    v = 0.95 * v + 0.05 * g * g
    step = m * lax.rsqrt(v + 1e-8) + 0.1 * w
    return (w - 0.02 * step).astype(jnp.bfloat16), m, v


def stack(weights, h):
    return lax.scan(lambda h, w: (layer(h, w), None), h, weights)[0]


def reference(x, dy, w_gate, w_up, w_down, m_w_gate, m_w_up, m_w_down, v_w_gate, v_w_up, v_w_down):
    weights = dict(zip(NAMES, (w_gate, w_up, w_down), strict=True))

    def take(so_far, sequence):
        h, by_y = sequence
        _, back = jax.vjp(lambda w: stack(w, h), weights)
        return jax.tree.map(lambda total, term: total + term.astype(jnp.float32), so_far, back(by_y)[0]), None

    none_yet = {name: jnp.zeros(w.shape, jnp.float32) for name, w in weights.items()}
    by_weights, _ = lax.scan(take, none_yet, (x, dy))
    gradients = [by_weights[name].astype(jnp.bfloat16).astype(jnp.float32) for name in NAMES]
    new = [
        adamw(w.astype(jnp.float32), m, v, g)
        for w, m, v, g in zip((w_gate, w_up, w_down), (m_w_gate, m_w_up, m_w_down), (v_w_gate, v_w_up, v_w_down), gradients, strict=True)
    ]
    return tuple(one[which] for which in range(3) for one in new)
```

```python
import jax
import jax.numpy as jnp
from jax import lax
from jax.sharding import PartitionSpec as P

NAMES = ("w_gate", "w_up", "w_down")


def dot(a, b, dims):
    return lax.dot_general(a, b, (dims, ((), ())), preferred_element_type=jnp.float32)


def normed(h):
    wide = h.astype(jnp.float32)
    scale = lax.rsqrt(jnp.mean(wide**2, -1, keepdims=True) + 1e-6)
    return (wide * scale).astype(jnp.bfloat16)


def halves(h, wg, wu):
    a = normed(h)
    gate, up = dot(a, wg, ((1,), (0,))), dot(a, wu, ((1,), (0,)))
    return a, gate, up


def of_mid(dmid, gate, up):
    s = jax.nn.sigmoid(gate)
    silu = gate * s
    wide = dmid.astype(jnp.float32)
    dup = wide * silu
    dgate = wide * up * (s * (1 + gate * (1 - s)))
    return dgate.astype(jnp.bfloat16), dup.astype(jnp.bfloat16)


def adamw(w, m, v, g):
    m = 0.9 * m + 0.1 * g
    v = 0.95 * v + 0.05 * g * g
    step = m * lax.rsqrt(v + 1e-8) + 0.1 * w
    return (w - 0.02 * step).astype(jnp.bfloat16), m, v


def solution(mesh):
    def body(x, dy, *arrays):
        weights, ms, vs = (dict(zip(NAMES, arrays[i : i + 3])) for i in (0, 3, 6))
        x, dy = x[0], dy[0]
        layers = weights["w_gate"].shape[0]
        me = lax.axis_index("dp")

        kept, h = [], x
        for n in range(layers):
            wg, wu, wd = (weights[k][n] for k in NAMES)
            a, gate, up = halves(h, wg, wu)
            mid = (jax.nn.silu(gate) * up).astype(jnp.bfloat16)
            kept.append((h, a, gate, up, mid))
            if n < layers - 1:
                h = h + dot(mid, wd, ((1,), (0,))).astype(jnp.bfloat16)

        new = {}

        def finish(k, n, g):
            g = lax.psum_scatter(g.astype(jnp.bfloat16), "dp", scatter_dimension=0, tiled=True)
            rows = g.shape[0]
            w = lax.dynamic_slice_in_dim(weights[k][n], me * rows, rows, 0)
            w, m, v = adamw(w.astype(jnp.float32), ms[k][n], vs[k][n], g.astype(jnp.float32))
            new[k, n] = lax.all_gather(w, "dp", axis=0, tiled=True), m, v

        d = dy
        for n in reversed(range(layers)):
            wg, wu, wd = (weights[k][n] for k in NAMES)
            h, a, gate, up, mid = kept[n]
            finish("w_down", n, dot(mid, d, ((0,), (0,))))
            dmid = dot(d, wd, ((1,), (1,))).astype(jnp.bfloat16)
            dgate, dup = of_mid(dmid, gate, up)
            finish("w_gate", n, dot(a, dgate, ((0,), (0,))))
            finish("w_up", n, dot(a, dup, ((0,), (0,))))
            if n:
                da = dot(dgate, wg, ((1,), (1,))).astype(jnp.bfloat16) + dot(dup, wu, ((1,), (1,))).astype(jnp.bfloat16)
                _, back = jax.vjp(normed, h)
                d = d + back(da)[0]
        return tuple(jnp.stack([new[k, n][i] for n in range(layers)]) for i in range(3) for k in NAMES)

    rows = P(None, "dp", None)
    seqs = P(("rep", "dp"), None, None)
    return jax.shard_map(
        body,
        mesh=mesh,
        in_specs=(seqs, seqs, P(), P(), P()) + (rows,) * 6,
        out_specs=(P("rep", None, None),) * 3 + (P("rep", "dp", None),) * 6,
        check_vma=False,
    )
```

```python
import functools

import jax
import jax.numpy as jnp
from jax import lax
from jax.experimental import pallas as pl
from jax.experimental.pallas import tpu as pltpu
from jax.sharding import PartitionSpec as P

NAMES = ("w_gate", "w_up", "w_down")
BF, F32 = jnp.bfloat16, jnp.float32
TILE = 512
LIMIT = 63_000_000


def dot(a, b, dims):
    return lax.dot_general(a, b, (dims, ((), ())), preferred_element_type=F32)


def normed(wide):
    return (wide * lax.rsqrt(jnp.mean(wide * wide, -1, keepdims=True) + 1e-6)).astype(BF)


def adamw(w, m, v, g):
    m = 0.9 * m + 0.1 * g
    v = 0.95 * v + 0.05 * g * g
    step = m * lax.rsqrt(v + 1e-8) + 0.1 * w
    return (w - 0.02 * step).astype(BF), m, v


def pieces(n, step):
    cuts = list(range(0, n - n % step, step)) + [n] if n % step else list(range(0, n + 1, step))
    if len(cuts) > 2 and cuts[-1] - cuts[-2] < step:
        del cuts[-2]
    return list(zip(cuts, cuts[1:]))


def whole(layer, rows, columns):
    return pl.BlockSpec((None, rows, columns), lambda t: (layer, 0, 0), pipeline_mode=pl.Buffered(1))


def tiles(columns):
    return pl.BlockSpec((TILE, columns), lambda t: (t, 0))


def forward(h, wg, wu, wd, layer):
    tokens, d = h.shape
    ff = wg.shape[-1]

    def kernel(h_ref, wg_ref, wu_ref, wd_ref, o_ref):
        wide = h_ref[...].astype(F32)
        a = normed(wide)
        total = jnp.zeros((TILE, d), F32)
        for lo, hi in pieces(ff, 768):
            gate = jnp.dot(a, wg_ref[:, lo:hi], preferred_element_type=F32)
            up = jnp.dot(a, wu_ref[:, lo:hi], preferred_element_type=F32)
            mid = (gate * jax.nn.sigmoid(gate) * up).astype(BF)
            total += jnp.dot(mid, wd_ref[lo:hi, :], preferred_element_type=F32)
        o_ref[...] = (wide + total.astype(BF).astype(F32)).astype(BF)

    return pl.pallas_call(
        kernel,
        grid=(tokens // TILE,),
        in_specs=[tiles(d), whole(layer, d, ff), whole(layer, d, ff), whole(layer, ff, d)],
        out_specs=tiles(d),
        out_shape=jax.ShapeDtypeStruct((tokens, d), BF),
        compiler_params=pltpu.CompilerParams(vmem_limit_bytes=LIMIT),
        cost_estimate=pl.CostEstimate(flops=6 * tokens * d * ff, bytes_accessed=2 * 3 * d * ff, transcendentals=tokens * ff),
        name="forward",
    )(h, wg, wu, wd)


def middles(h, dy, wg, wu, wd, layer):
    tokens, d = h.shape
    ff = wg.shape[-1]

    def kernel(h_ref, dy_ref, wg_ref, wu_ref, wd_ref, a_ref, o_ref):
        a = normed(h_ref[...].astype(F32))
        a_ref[...] = a
        dy = dy_ref[...]
        for lo, hi in pieces(ff, 768):
            gate = jnp.dot(a, wg_ref[:, lo:hi], preferred_element_type=F32)
            up = jnp.dot(a, wu_ref[:, lo:hi], preferred_element_type=F32)
            s = jax.nn.sigmoid(gate)
            silu = gate * s
            o_ref[2, :, lo:hi] = (silu * up).astype(BF)
            dmid = dot(dy, wd_ref[lo:hi, :], ((1,), (1,))).astype(BF).astype(F32)
            o_ref[0, :, lo:hi] = (dmid * up * (s * (1 + gate * (1 - s)))).astype(BF)
            o_ref[1, :, lo:hi] = (dmid * silu).astype(BF)

    return pl.pallas_call(
        kernel,
        grid=(tokens // TILE,),
        in_specs=[tiles(d), tiles(d), whole(layer, d, ff), whole(layer, d, ff), whole(layer, ff, d)],
        out_specs=[tiles(d), pl.BlockSpec((3, TILE, ff), lambda t: (0, t, 0))],
        out_shape=[jax.ShapeDtypeStruct((tokens, d), BF), jax.ShapeDtypeStruct((3, tokens, ff), BF)],
        compiler_params=pltpu.CompilerParams(vmem_limit_bytes=LIMIT),
        cost_estimate=pl.CostEstimate(flops=6 * tokens * d * ff, bytes_accessed=2 * 3 * (d + tokens) * ff, transcendentals=tokens * ff),
        name="middles",
    )(h, dy, wg, wu, wd)


def by_states(three, h, dy, wg, wu, layer):
    tokens, d = h.shape
    ff = wg.shape[-1]

    def kernel(t_ref, h_ref, dy_ref, wg_ref, wu_ref, o_ref):
        da = dot(t_ref[0], wg_ref[...], ((1,), (1,))).astype(BF) + dot(t_ref[1], wu_ref[...], ((1,), (1,))).astype(BF)
        da = da.astype(F32)
        wide = h_ref[...].astype(F32)
        scale = lax.rsqrt(jnp.mean(wide * wide, -1, keepdims=True) + 1e-6)
        inner = jnp.mean(da * wide, -1, keepdims=True)
        back = (da * scale - wide * (inner * scale * scale * scale)).astype(BF)
        o_ref[...] = (dy_ref[...].astype(F32) + back.astype(F32)).astype(BF)

    return pl.pallas_call(
        kernel,
        grid=(tokens // TILE,),
        in_specs=[pl.BlockSpec((2, TILE, ff), lambda t: (0, t, 0)), tiles(d), tiles(d), whole(layer, d, ff), whole(layer, d, ff)],
        out_specs=tiles(d),
        out_shape=jax.ShapeDtypeStruct((tokens, d), BF),
        compiler_params=pltpu.CompilerParams(vmem_limit_bytes=LIMIT),
        cost_estimate=pl.CostEstimate(flops=4 * tokens * d * ff, bytes_accessed=4 * (d + tokens) * ff, transcendentals=0),
        name="by_states",
    )(three, h, dy, wg, wu)


def summed(a, dy, three, size, collective_id):
    tokens, d = a.shape
    ff = three.shape[-1]
    chips, rows = size // 2, d // size
    assert chips == 4 and ff % d == 0 and ff // size % rows == 0 and d % size == 0
    cuts = ff // d
    blocks = 3 * cuts
    first = 48
    halves = (pl.ds(0, first), pl.ds(first, rows - first))
    late = cuts - 1
    lag0, lag1, lag2, lag3 = 1, 2, 4, 6
    steps = blocks + late + lag3

    def kernel(a_ref, dy_ref, t_ref, g_ref, u_ref, d_ref, own, near, out_a, out_b, in_a, in_b, send, recv):
        t = pl.program_id(0)
        me = lax.axis_index("dp")
        chip, core = me // 2, me % 2

        def at(step):
            return lax.rem(chip + step + chips, chips)

        def device(step):
            return {"dp": at(step) * 2 + core}

        def copy(src, dst, kind, q, to):
            return pltpu.make_async_remote_copy(
                src_ref=src, dst_ref=dst, send_sem=send.at[kind, q], recv_sem=recv.at[kind, q], device_id=to, device_id_type=pl.DeviceIdType.MESH
            )

        def way(q):
            return 1 - 2 * lax.rem(q, 2)

        def over(q):
            return copy(own.at[q, :, 1 - core], near.at[q], 0, q, {"dp": me + 1 - 2 * core})

        def message(q, kind, second):
            to = device(-way(q) if second == (kind != 1) else way(q))
            out, into = (out_b, in_b) if second else (out_a, in_a)
            return copy(out.at[q, kind], into.at[q, kind], 1 + 2 * kind + second, q, to)

        def part(q, c, half):
            return own[q, c, core, half, :].astype(F32) + near[q, c, half, :].astype(F32)

        def when(lag, f):
            e = t - lag
            on = jnp.logical_and(e >= 0, jnp.logical_or(e < 2 * cuts, jnp.logical_and(e >= 2 * cuts + late, e < blocks + late)))
            pl.when(on)(lambda: f(jnp.where(e < 2 * cuts, e, e - late)))

        @pl.when(t == 0)
        def _():
            barrier = pltpu.get_barrier_semaphore()
            for to in ({"dp": me + 1 - 2 * core}, device(1), device(-1)):
                pl.semaphore_signal(barrier, inc=1, device_id=to, device_id_type=pl.DeviceIdType.MESH)
            pl.semaphore_wait(barrier, 3)

        def finish(q):
            for kind in range(3):
                for second in (0, 1):
                    if kind:
                        message(q, kind, second).wait_recv()
            for second, into in ((0, in_a), (1, in_b)):
                half = halves[second]
                g = part(q, chip, half) + into[q, 1].astype(F32) + into[q, 2].astype(F32)
                g = g.astype(BF)
                at_column = pl.ds(pl.multiple_of(lax.rem(q, cuts) * d, 128), d)
                at_row = pl.ds(pl.multiple_of(lax.rem(q, cuts) * rows + half.start, 16), half.size)

                @pl.when(q < cuts)
                def _():
                    g_ref[half, at_column] = g

                @pl.when(jnp.logical_and(q >= cuts, q < 2 * cuts))
                def _():
                    u_ref[half, at_column] = g

                @pl.when(q >= 2 * cuts)
                def _():
                    d_ref[at_row, :] = g

            over(q).wait_send()
            for kind in range(3):
                for second in (0, 1):
                    message(q, kind, second).wait_send()

        def join(q):
            for second, out, into in ((0, out_a, in_a), (1, out_b, in_b)):
                message(q, 0, second).wait_recv()
                c = at(way(q) if second == 0 else -way(q))
                out[q, 2] = (part(q, c, halves[second]) + into[q, 0].astype(F32)).astype(BF)
            for second in (0, 1):
                message(q, 2, second).start()

        def split(q):
            over(q).wait_recv()
            for second, out in ((0, out_a), (1, out_b)):
                out[q, 0] = part(q, at(2), halves[second]).astype(BF)
                c = at(-way(q) if second == 0 else way(q))
                out[q, 1] = part(q, c, halves[second]).astype(BF)
            for kind in (0, 1):
                for second in (0, 1):
                    message(q, kind, second).start()

        when(lag0, lambda q: over(q).start())
        when(lag2, join)
        when(lag1, split)
        when(lag3, finish)

        @pl.when(t < 2 * cuts)
        def _():
            g = dot(a_ref[...], t_ref[...], ((0,), (0,))).astype(BF)
            own[t] = g.reshape(chips, 2, rows, d)

        @pl.when(jnp.logical_and(t >= 2 * cuts, t < blocks))
        def _():
            g = dot(t_ref[...], dy_ref[...], ((0,), (0,))).astype(BF)
            for p in range(size):
                n = (t - 2 * cuts) * size + p
                dev = n // cuts
                own[2 * cuts + lax.rem(n, cuts), dev // 2, lax.rem(dev, 2)] = g[p * rows : (p + 1) * rows]

    def block(t):
        t = jnp.minimum(t, blocks - 1)
        return t // cuts, 0, lax.rem(t, cuts)

    once = functools.partial(pl.BlockSpec, index_map=lambda t: (0, 0), pipeline_mode=pl.Buffered(1))
    second = rows - first
    return pl.pallas_call(
        kernel,
        grid=(steps,),
        in_specs=[once((tokens, d)), once((tokens, d)), pl.BlockSpec((None, tokens, d), block)],
        out_specs=[pl.BlockSpec((rows, ff), lambda t: (0, 0))] * 2 + [pl.BlockSpec((ff // size, d), lambda t: (0, 0))],
        out_shape=[jax.ShapeDtypeStruct((rows, ff), BF)] * 2 + [jax.ShapeDtypeStruct((ff // size, d), BF)],
        scratch_shapes=[
            pltpu.VMEM((blocks, chips, 2, rows, d), BF),
            pltpu.VMEM((blocks, chips, rows, d), BF),
            pltpu.VMEM((blocks, 3, first, d), BF),
            pltpu.VMEM((blocks, 3, second, d), BF),
            pltpu.VMEM((blocks, 3, first, d), BF),
            pltpu.VMEM((blocks, 3, second, d), BF),
            pltpu.SemaphoreType.DMA((7, blocks)),
            pltpu.SemaphoreType.DMA((7, blocks)),
        ],
        compiler_params=pltpu.CompilerParams(vmem_limit_bytes=LIMIT, collective_id=collective_id, has_side_effects=True),
        cost_estimate=pl.CostEstimate(flops=6 * tokens * d * ff, bytes_accessed=2 * 3 * tokens * ff, transcendentals=0),
        name="summed",
    )(a, dy, three)


def solution(mesh):
    size = mesh.shape["dp"]

    def body(x, dy, *arrays):
        weights, ms, vs = (dict(zip(NAMES, arrays[i : i + 3])) for i in (0, 3, 6))
        wg, wu, wd = (weights[k] for k in NAMES)
        states, d = [x[0]], dy[0]
        layers = wg.shape[0]
        me = lax.axis_index("dp")
        for n in range(layers - 1):
            states.append(forward(states[-1], wg, wu, wd, n))
        new = {}
        for n in reversed(range(layers)):
            a, three = middles(states[n], d, wg, wu, wd, n)
            sums = summed(a, d, three, size, n)
            if n:
                three, sums = lax.optimization_barrier((three, sums))
                d = by_states(three, states[n], d, wg, wu, n)
            for k, g in zip(NAMES, sums):
                rows = g.shape[0]
                w = lax.dynamic_slice_in_dim(weights[k][n], me * rows, rows, 0)
                w, m, v = adamw(w.astype(F32), ms[k][n], vs[k][n], g.astype(F32))
                new[k, n] = lax.all_gather(w, "dp", axis=0, tiled=True), m, v
        return tuple(jnp.stack([new[k, n][i] for n in range(layers)]) for i in range(3) for k in NAMES)

    rows = P(None, "dp", None)
    seqs = P(("rep", "dp"), None, None)
    return jax.shard_map(
        body,
        mesh=mesh,
        in_specs=(seqs, seqs, P(), P(), P()) + (rows,) * 6,
        out_specs=(P("rep", None, None),) * 3 + (P("rep", "dp", None),) * 6,
        check_vma=False,
    )
```

```python
import functools

import jax
import jax.numpy as jnp
from jax import lax
from jax.experimental import pallas as pl
from jax.experimental.pallas import tpu as pltpu
from jax.sharding import PartitionSpec as P

NAMES = ("w_gate", "w_up", "w_down")
BF, F32 = jnp.bfloat16, jnp.float32
TILE = 512
LIMIT = 66_900_000


def dot(a, b, dims):
    return lax.dot_general(a, b, (dims, ((), ())), preferred_element_type=F32)


def normed(wide):
    return (wide * lax.rsqrt(jnp.mean(wide * wide, -1, keepdims=True) + 1e-6)).astype(BF)


def adamw(w, m, v, g):
    m = 0.9 * m + 0.1 * g
    v = 0.95 * v + 0.05 * g * g
    step = m * lax.rsqrt(v + 1e-8) + 0.1 * w
    return (w - 0.02 * step).astype(BF), m, v


def pieces(n, step):
    cuts = list(range(0, n - n % step, step)) + [n] if n % step else list(range(0, n + 1, step))
    if len(cuts) > 2 and cuts[-1] - cuts[-2] < step:
        del cuts[-2]
    return list(zip(cuts, cuts[1:]))


def whole(layer, rows, columns):
    return pl.BlockSpec((None, rows, columns), lambda t: (layer, 0, 0), pipeline_mode=pl.Buffered(1))


def tiles(columns):
    return pl.BlockSpec((TILE, columns), lambda t: (t, 0))


def forward(h, wg, wu, wd, layer):
    tokens, d = h.shape
    ff = wg.shape[-1]

    def kernel(h_ref, wg_ref, wu_ref, wd_ref, o_ref):
        wide = h_ref[...].astype(F32)
        a = normed(wide)
        total = jnp.zeros((TILE, d), F32)
        for lo, hi in pieces(ff, 768):
            gate = jnp.dot(a, wg_ref[:, lo:hi], preferred_element_type=F32)
            up = jnp.dot(a, wu_ref[:, lo:hi], preferred_element_type=F32)
            mid = (gate * jax.nn.sigmoid(gate) * up).astype(BF)
            total += jnp.dot(mid, wd_ref[lo:hi, :], preferred_element_type=F32)
        o_ref[...] = (wide + total.astype(BF).astype(F32)).astype(BF)

    return pl.pallas_call(
        kernel,
        grid=(tokens // TILE,),
        in_specs=[tiles(d), whole(layer, d, ff), whole(layer, d, ff), whole(layer, ff, d)],
        out_specs=tiles(d),
        out_shape=jax.ShapeDtypeStruct((tokens, d), BF),
        compiler_params=pltpu.CompilerParams(vmem_limit_bytes=LIMIT),
        cost_estimate=pl.CostEstimate(flops=6 * tokens * d * ff, bytes_accessed=2 * 3 * d * ff, transcendentals=tokens * ff),
        name="forward",
    )(h, wg, wu, wd)


def by_states(three, h, dy, wg, wu, layer):
    tokens, d = h.shape
    ff = wg.shape[-1]

    def kernel(t_ref, h_ref, dy_ref, wg_ref, wu_ref, o_ref):
        da = dot(t_ref[0], wg_ref[...], ((1,), (1,))).astype(BF) + dot(t_ref[1], wu_ref[...], ((1,), (1,))).astype(BF)
        da = da.astype(F32)
        wide = h_ref[...].astype(F32)
        scale = lax.rsqrt(jnp.mean(wide * wide, -1, keepdims=True) + 1e-6)
        inner = jnp.mean(da * wide, -1, keepdims=True)
        back = (da * scale - wide * (inner * scale * scale * scale)).astype(BF)
        o_ref[...] = (dy_ref[...].astype(F32) + back.astype(F32)).astype(BF)

    return pl.pallas_call(
        kernel,
        grid=(tokens // TILE,),
        in_specs=[pl.BlockSpec((2, TILE, ff), lambda t: (0, t, 0)), tiles(d), tiles(d), whole(layer, d, ff), whole(layer, d, ff)],
        out_specs=tiles(d),
        out_shape=jax.ShapeDtypeStruct((tokens, d), BF),
        compiler_params=pltpu.CompilerParams(vmem_limit_bytes=LIMIT),
        cost_estimate=pl.CostEstimate(flops=4 * tokens * d * ff, bytes_accessed=4 * (d + tokens) * ff, transcendentals=0),
        name="by_states",
    )(three, h, dy, wg, wu)


def stepped(h, dy, weights, ms, vs, layer, size, through):
    tokens, d = h.shape
    ff = weights[0].shape[-1]
    chips, rows = size // 2, d // size
    assert chips == 4 and ff % d == 0 and ff // size % rows == 0 and d % size == 0
    cuts = ff // d
    blocks = 3 * cuts
    first = 48
    halves = (pl.ds(0, first), pl.ds(first, rows - first))
    tile = tokens // 4
    per = 7
    made = per * cuts
    lags = (1, 2, 4, 6, 8, 10, 12)
    steps = made + cuts + lags[-1]
    MESH = pl.DeviceIdType.MESH

    def kernel(h_ref, dy_ref, wg_ref, wu_ref, wd_ref, *rest):
        w_hbm, m_hbm, v_hbm = rest[:3], rest[3:6], rest[6:9]
        g_ref, all_ref, two, a_ref, mid, own, near, in_a, in_b, wnew, wold, mold, vold, send, recv, load, keep = rest[9:]
        t = pl.program_id(0)
        me = lax.axis_index("dp")
        chip, core = me // 2, me % 2
        partner = {"dp": me + 1 - 2 * core}

        def at(step):
            return lax.rem(chip + step + chips, chips)

        def dev(step):
            return at(step) * 2 + core

        def copy(src, dst, kind, q, to):
            return pltpu.make_async_remote_copy(
                src_ref=src, dst_ref=dst, send_sem=send.at[kind, q], recv_sem=recv.at[kind, q], device_id=to, device_id_type=MESH
            )

        def way(q):
            return 1 - 2 * lax.rem(q, 2)

        def over(q):
            return copy(own.at[q, :, 1 - core], near.at[q], 0, q, partner)

        def message(q, kind, second):
            step = -way(q) if second == (kind != 1) else way(q)
            c = at(2) if kind == 0 else at(step)
            into = in_b if second else in_a
            return copy(own.at[q, c, core, halves[second], :], into.at[q, kind], 1 + 2 * kind + second, q, {"dp": dev(step)})

        def part(q, c, half):
            return own[q, c, core, half, :].astype(F32) + near[q, c, half, :].astype(F32)

        def there(q, step):
            return copy(wnew.at[q], all_ref.at[q, me], 7 if step == 1 else 8, q, {"dp": dev(step)})

        def onward(q, second):
            step = -way(q) if second else way(q)
            where = all_ref.at[q, dev(-step), halves[second], :]
            return copy(where, where, 9 + second, q, {"dp": dev(step)})

        def across(q, step):
            where = all_ref.at[q, dev(step)]
            return copy(where if step else wnew.at[q], where, 11 + step + (step < 0) * 4, q, partner)

        def kept(q):
            return pltpu.make_async_copy(wnew.at[q], all_ref.at[q, me], keep.at[q])

        def slot(q):
            return jnp.where(q < 2 * cuts, lax.rem(q, 4), q - 2 * cuts + 4)

        def loads(q, which):
            n = slot(q)
            if which < 2:
                columns = pl.ds(pl.multiple_of(q // 2 * d, 128), d)
                mine, ours = (pl.ds(0, rows), columns), (pl.ds(pl.multiple_of(me * rows, 16), rows), columns)
            else:
                b = jnp.maximum(q - 2 * cuts, 0)
                mine = pl.ds(pl.multiple_of(b * rows, 16), rows), pl.ds(0, d)
                ours = pl.ds(pl.multiple_of(me * (ff // size) + b * rows, 16), rows), pl.ds(0, d)
            return (
                pltpu.make_async_copy(w_hbm[which].at[(layer, *ours)], wold.at[n], load.at[n, 0]),
                pltpu.make_async_copy(m_hbm[which].at[(layer, *mine)], mold.at[n], load.at[n, 1]),
                pltpu.make_async_copy(v_hbm[which].at[(layer, *mine)], vold.at[n], load.at[n, 2]),
            )

        @pl.when(t == 0)
        def _():
            barrier = pltpu.get_barrier_semaphore()
            for to in (partner, {"dp": dev(1)}, {"dp": dev(-1)}):
                pl.semaphore_signal(barrier, inc=1, device_id=to, device_id_type=MESH)
            pl.semaphore_wait(barrier, 3)

        def begin(q):
            over(q).start()
            for which, on in enumerate(
                (
                    jnp.logical_and(q < 2 * cuts, lax.rem(q, 2) == 0),
                    jnp.logical_and(q < 2 * cuts, lax.rem(q, 2) == 1),
                    q >= 2 * cuts,
                )
            ):

                @pl.when(on)
                def _(which=which):
                    for one in loads(q, which):
                        one.start()

        def split(q):
            over(q).wait()
            for kind in (0, 1):
                for second in (0, 1):
                    step = -way(q) if second == (kind != 1) else way(q)
                    c = at(2) if kind == 0 else at(step)
                    own[q, c, core, halves[second], :] = part(q, c, halves[second]).astype(BF)
            for kind in (0, 1):
                for second in (0, 1):
                    message(q, kind, second).start()

        def join(q):
            for second, into in ((0, in_a), (1, in_b)):
                message(q, 0, second).wait_recv()
                c = at(-way(q) if second else way(q))
                own[q, c, core, halves[second], :] = (part(q, c, halves[second]) + into[q, 0].astype(F32)).astype(BF)
            for second in (0, 1):
                message(q, 2, second).start()

        def update(q):
            for kind in (1, 2):
                for second in (0, 1):
                    message(q, kind, second).wait_recv()
            for one in loads(q, 2):
                one.wait()
            n = slot(q)
            for second, into in ((0, in_a), (1, in_b)):
                half = halves[second]
                g = (part(q, chip, half) + into[q, 1].astype(F32) + into[q, 2].astype(F32)).astype(BF)
                g_ref[q, half, :] = g
                wnew[q, half, :] = adamw(wold[n, half, :].astype(F32), mold[n, half, :], vold[n, half, :], g.astype(F32))[0]
            there(q, 1).start()
            there(q, -1).start()
            across(q, 0).start()
            kept(q).start()

        def relay(q):
            there(q, 1).wait_recv()
            there(q, -1).wait_recv()
            onward(q, 0).start()
            onward(q, 1).start()
            across(q, 1).start()
            across(q, -1).start()

        def rest_of(q):
            onward(q, 0).wait_recv()
            onward(q, 1).wait_recv()
            across(q, 2).start()

        def close(q):
            for step in (0, 1, -1, 2):
                across(q, step).wait()
            kept(q).wait()
            for kind in range(3):
                for second in (0, 1):
                    message(q, kind, second).wait_send()
            there(q, 1).wait_send()
            there(q, -1).wait_send()
            onward(q, 0).wait_send()
            onward(q, 1).wait_send()

        for lag, act in reversed(tuple(zip(lags, (begin, split, join, update, relay, rest_of, close)))):
            late = t - lag - made + 1
            pl.when(jnp.logical_and(late >= 0, late < cuts))(functools.partial(act, 2 * cuts + late))
            e = t - lag
            r = lax.rem(e, per)
            on = jnp.logical_and(jnp.logical_and(e >= 0, e < made), jnp.logical_and(r >= per - 3, r < per - 1))
            pl.when(on)(functools.partial(act, 2 * (e // per) + r - (per - 3)))

        b, r = t // per, lax.rem(t, per)

        @pl.when(jnp.logical_and(t < made, r < per - 3))
        def _():
            here = pl.ds(pl.multiple_of(r * tile, tile), tile)

            @pl.when(b == 0)
            def _():
                a_ref[here, :] = normed(h_ref[here, :].astype(F32))

            a = a_ref[here, :]
            gate = jnp.dot(a, wg_ref[...], preferred_element_type=F32)
            up = jnp.dot(a, wu_ref[...], preferred_element_type=F32)
            s = jax.nn.sigmoid(gate)
            silu = gate * s
            mid[here, :] = (silu * up).astype(BF)
            dmid = dot(dy_ref[here, :], wd_ref[...], ((1,), (1,))).astype(BF).astype(F32)
            two[0, here, :] = (dmid * up * (s * (1 + gate * (1 - s)))).astype(BF)
            two[1, here, :] = (dmid * silu).astype(BF)

        @pl.when(jnp.logical_and(t < made, jnp.logical_and(r >= per - 3, r < per - 1)))
        def _():
            g = dot(a_ref[...], two[r - (per - 3)], ((0,), (0,))).astype(BF)
            own[2 * b + r - (per - 3)] = g.reshape(chips, 2, rows, d)

        @pl.when(jnp.logical_and(t < made, r == per - 1))
        def _():
            g = dot(mid[...], dy_ref[...], ((0,), (0,))).astype(BF)
            for p in range(size):
                n = b * size + p
                owner = n // cuts
                own[2 * cuts + lax.rem(n, cuts), owner // 2, lax.rem(owner, 2)] = g[p * rows : (p + 1) * rows]

    def block(t):
        return jnp.minimum(t // per, cuts - 1)

    once = functools.partial(pl.BlockSpec, index_map=lambda t: (0, 0), pipeline_mode=pl.Buffered(1))
    wide = pl.BlockSpec((None, d, d), lambda t: (layer, 0, block(t)))
    tall = pl.BlockSpec((None, d, d), lambda t: (layer, block(t), 0))
    hbm = pl.BlockSpec(memory_space=pl.ANY)
    second = rows - first
    two = pl.BlockSpec((2, tokens, d), lambda t: (0, 0, block(t)))
    out_specs = [pl.BlockSpec((blocks, rows, d), lambda t: (0, 0, 0)), hbm]
    out_shape = [jax.ShapeDtypeStruct((blocks, rows, d), BF), jax.ShapeDtypeStruct((blocks, size, rows, d), BF)]
    scratch = [] if through else [pltpu.VMEM((2, tokens, d), BF)]
    return pl.pallas_call(
        kernel,
        grid=(steps,),
        in_specs=[once((tokens, d)), once((tokens, d)), wide, wide, tall] + [hbm] * 9,
        out_specs=out_specs + [two] * through,
        out_shape=out_shape + [jax.ShapeDtypeStruct((2, tokens, ff), BF)] * through,
        scratch_shapes=scratch
        + [
            pltpu.VMEM((tokens, d), BF),
            pltpu.VMEM((tokens, d), BF),
            pltpu.VMEM((blocks, chips, 2, rows, d), BF),
            pltpu.VMEM((blocks, chips, rows, d), BF),
            pltpu.VMEM((blocks, 3, first, d), BF),
            pltpu.VMEM((blocks, 3, second, d), BF),
            pltpu.VMEM((blocks, rows, d), BF),
            pltpu.VMEM((4 + cuts, rows, d), BF),
            pltpu.VMEM((4 + cuts, rows, d), F32),
            pltpu.VMEM((4 + cuts, rows, d), F32),
            pltpu.SemaphoreType.DMA((15, blocks)),
            pltpu.SemaphoreType.DMA((15, blocks)),
            pltpu.SemaphoreType.DMA((4 + cuts, 3)),
            pltpu.SemaphoreType.DMA((blocks,)),
        ],
        compiler_params=pltpu.CompilerParams(vmem_limit_bytes=LIMIT, collective_id=layer, has_side_effects=True),
        cost_estimate=pl.CostEstimate(flops=12 * tokens * d * ff, bytes_accessed=2 * 3 * tokens * ff, transcendentals=0),
        name="stepped",
    )(h, dy, *weights, *weights, *ms, *vs)


def solution(mesh):
    size = mesh.shape["dp"]

    def body(x, dy, *arrays):
        weights, ms, vs = (arrays[i : i + 3] for i in (0, 3, 6))
        wg, wu, wd = weights
        states, d = [x[0]], dy[0]
        layers, width, ff = wg.shape
        rows = width // size
        cuts = ff // width
        me = lax.axis_index("dp")
        for n in range(layers - 1):
            states.append(forward(states[-1], wg, wu, wd, n))
        sums, gathered = [None] * layers, [None] * layers
        for n in reversed(range(layers)):
            sums[n], gathered[n], *two = stepped(states[n], d, weights, ms, vs, n, size, n > 0)
            if n:
                d = by_states(two[0], states[n], d, wg, wu, n)

        def wide(t):
            return jnp.moveaxis(t, 0, -2).reshape(-1, ff)

        def tall(t):
            return jnp.moveaxis(t, 0, -3).reshape(-1, width)

        def each(t):
            return wide(t[0 : 2 * cuts : 2]), wide(t[1 : 2 * cuts : 2]), tall(t[2 * cuts :])

        out = [jnp.stack(one) for one in zip(*map(each, gathered))]
        totals = [jnp.stack(one) for one in zip(*map(each, sums))]
        moments = []
        for w, m, v, g in zip(weights, ms, vs, totals):
            moments.append(adamw(jnp.zeros_like(m), m, v, g.astype(F32))[1:])
        return (*out, *(m for m, _ in moments), *(v for _, v in moments))

    rows = P(None, "dp", None)
    seqs = P(("rep", "dp"), None, None)
    return jax.shard_map(
        body,
        mesh=mesh,
        in_specs=(seqs, seqs, P(), P(), P()) + (rows,) * 6,
        out_specs=(P("rep", None, None),) * 3 + (P("rep", "dp", None),) * 6,
        check_vma=False,
    )
```

```python
import functools

import jax
import jax.numpy as jnp
from jax import lax
from jax.experimental import pallas as pl
from jax.experimental.pallas import tpu as pltpu
from jax.sharding import PartitionSpec as P

NAMES = ("w_gate", "w_up", "w_down")
BF, F32 = jnp.bfloat16, jnp.float32
TILE = 512
LIMIT = 66_900_000


def dot(a, b, dims):
    return lax.dot_general(a, b, (dims, ((), ())), preferred_element_type=F32)


def normed(wide):
    return (wide * lax.rsqrt(jnp.mean(wide * wide, -1, keepdims=True) + 1e-6)).astype(BF)


def adamw(w, m, v, g):
    m = 0.9 * m + 0.1 * g
    v = 0.95 * v + 0.05 * g * g
    step = m * lax.rsqrt(v + 1e-8) + 0.1 * w
    return (w - 0.02 * step).astype(BF), m, v


def pieces(n, step):
    cuts = list(range(0, n - n % step, step)) + [n] if n % step else list(range(0, n + 1, step))
    if len(cuts) > 2 and cuts[-1] - cuts[-2] < step:
        del cuts[-2]
    return list(zip(cuts, cuts[1:]))


def whole(layer, rows, columns):
    return pl.BlockSpec((None, rows, columns), lambda t: (layer, 0, 0), pipeline_mode=pl.Buffered(1))


def tiles(columns):
    return pl.BlockSpec((TILE, columns), lambda t: (t, 0))


def forward(h, wg, wu, wd, layer):
    tokens, d = h.shape
    ff = wg.shape[-1]

    def kernel(h_ref, wg_ref, wu_ref, wd_ref, o_ref, mid_ref):
        wide = h_ref[...].astype(F32)
        a = normed(wide)
        total = jnp.zeros((TILE, d), F32)
        for lo, hi in pieces(ff, 768):
            gate = jnp.dot(a, wg_ref[:, lo:hi], preferred_element_type=F32)
            up = jnp.dot(a, wu_ref[:, lo:hi], preferred_element_type=F32)
            mid = (gate * jax.nn.sigmoid(gate) * up).astype(BF)
            mid_ref[:, lo:hi] = mid
            total += jnp.dot(mid, wd_ref[lo:hi, :], preferred_element_type=F32)
        o_ref[...] = (wide + total.astype(BF).astype(F32)).astype(BF)

    return pl.pallas_call(
        kernel,
        grid=(tokens // TILE,),
        in_specs=[tiles(d), whole(layer, d, ff), whole(layer, d, ff), whole(layer, ff, d)],
        out_specs=[tiles(d), tiles(ff)],
        out_shape=[jax.ShapeDtypeStruct((tokens, d), BF), jax.ShapeDtypeStruct((tokens, ff), BF)],
        compiler_params=pltpu.CompilerParams(vmem_limit_bytes=LIMIT),
        cost_estimate=pl.CostEstimate(flops=6 * tokens * d * ff, bytes_accessed=2 * 3 * d * ff, transcendentals=tokens * ff),
        name="forward",
    )(h, wg, wu, wd)


def stepped(x, h, mid0, dy, weights, ms, vs, size):
    tokens, d = h.shape
    layers, _, ff = weights[0].shape
    chips, rows = size // 2, d // size
    assert layers == 2 and chips == 4 and ff % d == 0 and ff // size % rows == 0 and d % size == 0
    cuts = ff // d
    blocks = 3 * cuts
    slots = 4 + cuts
    first = 48
    second = rows - first
    halves = (pl.ds(0, first), pl.ds(first, second))
    parts = 4
    tile = tokens // parts
    per = parts + 3
    lags = (1, 2, 4, 6, 8, 10, 12)
    made = per * cuts
    states_at = made
    down_at = states_at + parts * cuts
    again_at = down_at + cuts
    steps = again_at + made - 1 + lags[-1]
    MESH = pl.DeviceIdType.MESH

    def kernel(x_ref, h_ref, dy_ref, wg_ref, wu_ref, wd_ref, mid0_hbm, *rest):
        w_hbm, m_hbm, v_hbm = rest[:3], rest[3:6], rest[6:9]
        g_hbm, all_ref, two_hbm = rest[9:12]
        two, a_ref, a_t, dy_all, dy_t, mid, taken, by_g, by_u = rest[12:21]
        own, near, in_a, in_b, gnew, wnew, wold, mold, vold, send, recv, load, keep, away, fetch = rest[21:]
        t = pl.program_id(0)
        me = lax.axis_index("dp")
        chip, core = me // 2, me % 2
        partner = {"dp": me + 1 - 2 * core}

        def at(step):
            return lax.rem(chip + step + chips, chips)

        def dev(step):
            return at(step) * 2 + core

        def slot(q):
            return jnp.where(q < 2 * cuts, lax.rem(q, 4), q - 2 * cuts + 4)

        def copy(src, dst, kind, q, to):
            n = slot(q)
            return pltpu.make_async_remote_copy(
                src_ref=src, dst_ref=dst, send_sem=send.at[kind, n], recv_sem=recv.at[kind, n], device_id=to, device_id_type=MESH
            )

        def way(q):
            return 1 - 2 * lax.rem(q, 2)

        def over(q):
            return copy(own.at[slot(q), :, 1 - core], near.at[slot(q)], 0, q, partner)

        def message(q, kind, second):
            step = -way(q) if second == (kind != 1) else way(q)
            c = at(2) if kind == 0 else at(step)
            into = in_b if second else in_a
            return copy(own.at[slot(q), c, core, halves[second], :], into.at[slot(q), kind], 1 + 2 * kind + second, q, {"dp": dev(step)})

        def part(q, c, half):
            return own[slot(q), c, core, half, :].astype(F32) + near[slot(q), c, half, :].astype(F32)

        def there(n, q, step):
            return copy(wnew.at[slot(q)], all_ref.at[n, q, me], 7 if step == 1 else 8, q, {"dp": dev(step)})

        def onward(n, q, second):
            step = -way(q) if second else way(q)
            where = all_ref.at[n, q, dev(-step), halves[second], :]
            return copy(where, where, 9 + second, q, {"dp": dev(step)})

        def across(n, q, step):
            where = all_ref.at[n, q, dev(step)]
            return copy(where if step else wnew.at[slot(q)], where, 11 + step + (step < 0) * 4, q, partner)

        def kept(n, q):
            return (
                pltpu.make_async_copy(wnew.at[slot(q)], all_ref.at[n, q, me], keep.at[slot(q), 0]),
                pltpu.make_async_copy(gnew.at[slot(q)], g_hbm.at[n, q], keep.at[slot(q), 1]),
            )

        def loads(n, q, which):
            k = slot(q)
            if which < 2:
                columns = pl.ds(pl.multiple_of(q // 2 * d, 128), d)
                mine, ours = (pl.ds(0, rows), columns), (pl.ds(pl.multiple_of(me * rows, 16), rows), columns)
            else:
                b = jnp.maximum(q - 2 * cuts, 0)
                mine = pl.ds(pl.multiple_of(b * rows, 16), rows), pl.ds(0, d)
                ours = pl.ds(pl.multiple_of(me * (ff // size) + b * rows, 16), rows), pl.ds(0, d)
            return (
                pltpu.make_async_copy(w_hbm[which].at[(n, *ours)], wold.at[k], load.at[k, 0]),
                pltpu.make_async_copy(m_hbm[which].at[(n, *mine)], mold.at[k], load.at[k, 1]),
                pltpu.make_async_copy(v_hbm[which].at[(n, *mine)], vold.at[k], load.at[k, 2]),
            )

        @pl.when(t == 0)
        def _():
            barrier = pltpu.get_barrier_semaphore()
            for to in (partner, {"dp": dev(1)}, {"dp": dev(-1)}):
                pl.semaphore_signal(barrier, inc=1, device_id=to, device_id_type=MESH)
            pl.semaphore_wait(barrier, 3)

        def begin(n, q):
            over(q).start()
            for which, on in enumerate(
                (
                    jnp.logical_and(q < 2 * cuts, lax.rem(q, 2) == 0),
                    jnp.logical_and(q < 2 * cuts, lax.rem(q, 2) == 1),
                    q >= 2 * cuts,
                )
            ):

                @pl.when(on)
                def _(which=which):
                    for one in loads(n, q, which):
                        one.start()

        def split(n, q):
            over(q).wait()
            for kind in (0, 1):
                for second in (0, 1):
                    step = -way(q) if second == (kind != 1) else way(q)
                    c = at(2) if kind == 0 else at(step)
                    own[slot(q), c, core, halves[second], :] = part(q, c, halves[second]).astype(BF)
            for kind in (0, 1):
                for second in (0, 1):
                    message(q, kind, second).start()

        def join(n, q):
            for second, into in ((0, in_a), (1, in_b)):
                message(q, 0, second).wait_recv()
                c = at(-way(q) if second else way(q))
                total = part(q, c, halves[second]) + into[slot(q), 0].astype(F32)
                own[slot(q), c, core, halves[second], :] = total.astype(BF)
            for second in (0, 1):
                message(q, 2, second).start()

        def update(n, q):
            for kind in (1, 2):
                for second in (0, 1):
                    message(q, kind, second).wait_recv()
            for one in loads(n, q, 2):
                one.wait()
            k = slot(q)
            for second, into in ((0, in_a), (1, in_b)):
                half = halves[second]
                g = (part(q, chip, half) + into[k, 1].astype(F32) + into[k, 2].astype(F32)).astype(BF)
                gnew[k, half, :] = g
                wnew[k, half, :] = adamw(wold[k, half, :].astype(F32), mold[k, half, :], vold[k, half, :], g.astype(F32))[0]
            there(n, q, 1).start()
            there(n, q, -1).start()
            across(n, q, 0).start()
            for one in kept(n, q):
                one.start()

        def relay(n, q):
            there(n, q, 1).wait_recv()
            there(n, q, -1).wait_recv()
            onward(n, q, 0).start()
            onward(n, q, 1).start()
            across(n, q, 1).start()
            across(n, q, -1).start()

        def rest_of(n, q):
            onward(n, q, 0).wait_recv()
            onward(n, q, 1).wait_recv()
            across(n, q, 2).start()

        def close(n, q):
            for step in (0, 1, -1, 2):
                across(n, q, step).wait()
            for one in kept(n, q):
                one.wait()
            for kind in range(3):
                for second in (0, 1):
                    message(q, kind, second).wait_send()
            there(n, q, 1).wait_send()
            there(n, q, -1).wait_send()
            onward(n, q, 0).wait_send()
            onward(n, q, 1).wait_send()

        def inside(e, lo, hi):
            return jnp.logical_and(e >= lo, e < hi)

        for lag, act in reversed(tuple(zip(lags, (begin, split, join, update, relay, rest_of, close)))):
            e = t - lag
            n = jnp.where(e < again_at - 1, 1, 0)
            late = e - jnp.where(n == 1, made - 1, again_at - 1)
            pl.when(inside(late, 0, cuts))(functools.partial(act, n, 2 * cuts + late))
            n = jnp.where(e < again_at, 1, 0)
            e = e - jnp.where(n == 1, 0, again_at)
            r = lax.rem(e, per)
            pl.when(jnp.logical_and(inside(e, 0, made), inside(r, parts, parts + 2)))(functools.partial(act, n, 2 * (e // per) + r - parts))

        last = t < states_at
        i = t - jnp.where(last, 0, again_at)
        b, r = i // per, lax.rem(i, per)
        on = inside(i, 0, made)

        def out_copy(b):
            return pltpu.make_async_copy(two, two_hbm.at[:, :, pl.ds(pl.multiple_of(b * d, 128), d)], away)

        def fetched(i):
            where = two_hbm.at[:, pl.ds(pl.multiple_of(i // cuts * tile, tile), tile), pl.ds(pl.multiple_of(lax.rem(i, cuts) * d, 128), d)]
            return pltpu.make_async_copy(where, taken.at[lax.rem(i, 2)], fetch.at[lax.rem(i, 2)])

        def product(i):
            where = mid0_hbm.at[:, pl.ds(pl.multiple_of(i * d, 128), d)]
            return pltpu.make_async_copy(where, two.at[lax.rem(i, 2)], fetch.at[lax.rem(i, 2)])

        def spread(g, b):
            for p in range(size):
                n = b * size + p
                owner = n // cuts
                own[4 + lax.rem(n, cuts), owner // 2, lax.rem(owner, 2)] = g[p * rows : (p + 1) * rows]

        @pl.when(jnp.logical_and(last, jnp.logical_and(r == 0, b > 0)))
        def _():
            out_copy(b - 1).wait()

        @pl.when(jnp.logical_and(on, r < parts))
        def _():
            here = pl.ds(pl.multiple_of(r * tile, tile), tile)

            @pl.when(b == 0)
            def _():
                @pl.when(last)
                def _():
                    a_ref[here, :] = normed(h_ref[...].astype(F32))
                    dy_all[here, :] = dy_ref[...]
                    dy_t[:, here] = dy_ref[...].T

                @pl.when(jnp.logical_not(last))
                def _():
                    a_ref[here, :] = normed(x_ref[...].astype(F32))

                a_t[:, here] = a_ref[here, :].T

            a = a_ref[here, :]
            gate = jnp.dot(a, wg_ref[...], preferred_element_type=F32)
            up = jnp.dot(a, wu_ref[...], preferred_element_type=F32)
            s = jax.nn.sigmoid(gate)
            silu = gate * s
            mid[here, :] = (silu * up).astype(BF)
            dmid = dot(dy_all[here, :], wd_ref[...], ((1,), (1,))).astype(BF).astype(F32)
            two[0, here, :] = (dmid * up * (s * (1 + gate * (1 - s)))).astype(BF)
            two[1, here, :] = (dmid * silu).astype(BF)

            @pl.when(jnp.logical_and(last, r == parts - 1))
            def _():
                out_copy(b).start()

        @pl.when(jnp.logical_and(on, inside(r, parts, parts + 2)))
        def _():
            g = jnp.dot(a_t[...], two[r - parts], preferred_element_type=F32).astype(BF)
            own[slot(2 * b + r - parts)] = g.reshape(chips, 2, rows, d)

        @pl.when(jnp.logical_and(last, r == per - 1))
        def _():
            spread(jnp.dot(dy_t[...], mid[...], preferred_element_type=F32).astype(BF).T, b)

        @pl.when(t == states_at - 1)
        def _():
            out_copy(cuts - 1).wait()
            fetched(0).start()

        j = t - states_at

        @pl.when(inside(j, 0, parts * cuts))
        def _():
            k = lax.rem(j, cuts)
            fetched(j).wait()

            @pl.when(j < parts * cuts - 1)
            def _():
                fetched(j + 1).start()

            @pl.when(j == parts * cuts - 1)
            def _():
                product(0).start()

            at_g = dot(taken[lax.rem(j, 2), 0], wg_ref[...], ((1,), (1,)))
            at_u = dot(taken[lax.rem(j, 2), 1], wu_ref[...], ((1,), (1,)))

            @pl.when(k == 0)
            def _():
                by_g[...] = at_g
                by_u[...] = at_u

            @pl.when(k > 0)
            def _():
                by_g[...] += at_g
                by_u[...] += at_u

            @pl.when(k == cuts - 1)
            def _():
                here = pl.ds(pl.multiple_of(j // cuts * tile, tile), tile)
                da = (by_g[...].astype(BF).astype(F32) + by_u[...].astype(BF).astype(F32)).astype(BF).astype(F32)
                wide = h_ref[...].astype(F32)
                scale = lax.rsqrt(jnp.mean(wide * wide, -1, keepdims=True) + 1e-6)
                inner = jnp.mean(da * wide, -1, keepdims=True)
                back = (da * scale - wide * (inner * scale * scale * scale)).astype(BF)
                new = (dy_all[here, :].astype(F32) + back.astype(F32)).astype(BF)
                dy_all[here, :] = new
                dy_t[:, here] = new.T

        @pl.when(inside(t, down_at, again_at))
        def _():
            k = t - down_at
            product(k).wait()

            @pl.when(k < cuts - 1)
            def _():
                product(k + 1).start()

            spread(jnp.dot(dy_t[...], two[lax.rem(k, 2)], preferred_element_type=F32).astype(BF).T, k)

    def block(t):
        again = jnp.clip(jnp.maximum(t - again_at, 0) // per, 0, cuts - 1)
        b = jnp.where(t < states_at, t // per, jnp.where(t < down_at, lax.rem(jnp.maximum(t - states_at, 0), cuts), again))
        return jnp.where(t < down_at, 1, 0), b

    def at_states(t):
        return jnp.where(t < states_at, jnp.minimum(t, parts - 1), jnp.minimum((t - states_at) // cuts, parts - 1)), 0

    wide = pl.BlockSpec((None, d, d), lambda t: (block(t)[0], 0, block(t)[1]))
    tall = pl.BlockSpec((None, d, d), lambda t: (*block(t), 0))
    hbm = pl.BlockSpec(memory_space=pl.ANY)
    return pl.pallas_call(
        kernel,
        grid=(steps,),
        in_specs=[
            pl.BlockSpec((tile, d), lambda t: (jnp.clip(t - again_at, 0, parts - 1), 0)),
            pl.BlockSpec((tile, d), at_states),
            pl.BlockSpec((tile, d), lambda t: (jnp.minimum(t, parts - 1), 0)),
            wide,
            wide,
            tall,
        ]
        + [hbm] * 10,
        out_specs=[hbm] * 3,
        out_shape=[
            jax.ShapeDtypeStruct((layers, blocks, rows, d), BF),
            jax.ShapeDtypeStruct((layers, blocks, size, rows, d), BF),
            jax.ShapeDtypeStruct((2, tokens, ff), BF),
        ],
        scratch_shapes=[
            pltpu.VMEM((2, tokens, d), BF),
            pltpu.VMEM((tokens, d), BF),
            pltpu.VMEM((d, tokens), BF),
            pltpu.VMEM((tokens, d), BF),
            pltpu.VMEM((d, tokens), BF),
            pltpu.VMEM((tokens, d), BF),
            pltpu.VMEM((2, 2, tile, d), BF),
            pltpu.VMEM((tile, d), F32),
            pltpu.VMEM((tile, d), F32),
            pltpu.VMEM((slots, chips, 2, rows, d), BF),
            pltpu.VMEM((slots, chips, rows, d), BF),
            pltpu.VMEM((slots, 3, first, d), BF),
            pltpu.VMEM((slots, 3, second, d), BF),
            pltpu.VMEM((slots, rows, d), BF),
            pltpu.VMEM((slots, rows, d), BF),
            pltpu.VMEM((slots, rows, d), BF),
            pltpu.VMEM((slots, rows, d), F32),
            pltpu.VMEM((slots, rows, d), F32),
            pltpu.SemaphoreType.DMA((15, slots)),
            pltpu.SemaphoreType.DMA((15, slots)),
            pltpu.SemaphoreType.DMA((slots, 3)),
            pltpu.SemaphoreType.DMA((slots, 2)),
            pltpu.SemaphoreType.DMA,
            pltpu.SemaphoreType.DMA((2,)),
        ],
        compiler_params=pltpu.CompilerParams(vmem_limit_bytes=LIMIT, collective_id=0, has_side_effects=True),
        cost_estimate=pl.CostEstimate(flops=26 * tokens * d * ff, bytes_accessed=4 * 3 * tokens * ff, transcendentals=0),
        name="stepped",
    )(x, h, dy, *weights, mid0, *weights, *ms, *vs)


def assembled(gathered):
    layers, blocks, size, rows, d = gathered.shape
    cuts = blocks // 3
    ff = cuts * d

    def kernel(ref, g_ref, u_ref, d_ref):
        for p in range(2):
            for b in range(cuts):
                g_ref[p * rows : (p + 1) * rows, b * d : (b + 1) * d] = ref[2 * b, p]
                u_ref[p * rows : (p + 1) * rows, b * d : (b + 1) * d] = ref[2 * b + 1, p]
                d_ref[(p * cuts + b) * rows : (p * cuts + b + 1) * rows, :] = ref[2 * cuts + b, p]

    wide = pl.BlockSpec((None, 2 * rows, ff), lambda n, p: (n, p, 0))
    tall = pl.BlockSpec((None, 2 * ff // size, d), lambda n, p: (n, p, 0))
    return pl.pallas_call(
        kernel,
        grid=(layers, size // 2),
        in_specs=[pl.BlockSpec((None, blocks, 2, rows, d), lambda n, p: (n, 0, p, 0, 0))],
        out_specs=[wide, wide, tall],
        out_shape=[jax.ShapeDtypeStruct((layers, d, ff), BF)] * 2 + [jax.ShapeDtypeStruct((layers, ff, d), BF)],
        name="assembled",
    )(gathered)


def moments(sums, ms, vs):
    layers, blocks, rows, d = sums.shape
    cuts = blocks // 3

    def kernel(g_ref, *refs):
        b = pl.program_id(1)
        for i, q in enumerate((2 * b, 2 * b + 1, 2 * cuts + b)):
            g = g_ref[q].astype(F32)
            _, refs[6 + i][...], refs[9 + i][...] = adamw(jnp.zeros_like(g), refs[i][...], refs[3 + i][...], g)

    wide = pl.BlockSpec((None, rows, d), lambda n, b: (n, 0, b))
    tall = pl.BlockSpec((None, rows, d), lambda n, b: (n, b, 0))
    return pl.pallas_call(
        kernel,
        grid=(layers, cuts),
        in_specs=[pl.BlockSpec((None, blocks, rows, d), lambda n, b: (n, 0, 0, 0))] + [wide, wide, tall] * 2,
        out_specs=[wide, wide, tall] * 2,
        out_shape=[jax.ShapeDtypeStruct(t.shape, F32) for t in ms] * 2,
        name="moments",
    )(sums, *ms, *vs)


def solution(mesh):
    size = mesh.shape["dp"]

    def body(x, dy, *arrays):
        weights, ms, vs = (arrays[i : i + 3] for i in (0, 3, 6))
        h, mid0 = forward(x[0], *weights, 0)
        sums, gathered, _ = stepped(x[0], h, mid0, dy[0], weights, ms, vs, size)
        return (*assembled(gathered), *moments(sums, ms, vs))

    rows = P(None, "dp", None)
    seqs = P(("rep", "dp"), None, None)
    return jax.shard_map(
        body,
        mesh=mesh,
        in_specs=(seqs, seqs, P(), P(), P()) + (rows,) * 6,
        out_specs=(P("rep", None, None),) * 3 + (P("rep", "dp", None),) * 6,
        check_vma=False,
    )
```

```python
import functools

import jax
import jax.numpy as jnp
from jax import lax
from jax.experimental import pallas as pl
from jax.experimental.pallas import tpu as pltpu
from jax.sharding import PartitionSpec as P

NAMES = ("w_gate", "w_up", "w_down")
BF, F32 = jnp.bfloat16, jnp.float32
TILE = 512
LIMIT = 66_900_000


def dot(a, b, dims):
    return lax.dot_general(a, b, (dims, ((), ())), preferred_element_type=F32)


def normed(wide):
    return (wide * lax.rsqrt(jnp.mean(wide * wide, -1, keepdims=True) + 1e-6)).astype(BF)


def adamw(w, m, v, g):
    m = 0.9 * m + 0.1 * g
    v = 0.95 * v + 0.05 * g * g
    step = m * lax.rsqrt(v + 1e-8) + 0.1 * w
    return (w - 0.02 * step).astype(BF), m, v


def pieces(n, step):
    cuts = list(range(0, n - n % step, step)) + [n] if n % step else list(range(0, n + 1, step))
    if len(cuts) > 2 and cuts[-1] - cuts[-2] < step:
        del cuts[-2]
    return list(zip(cuts, cuts[1:]))


def whole(layer, rows, columns):
    return pl.BlockSpec((None, rows, columns), lambda t: (layer, 0, 0), pipeline_mode=pl.Buffered(1))


def tiles(columns):
    return pl.BlockSpec((TILE, columns), lambda t: (t, 0))


def forward(h, wg, wu, wd, layer):
    tokens, d = h.shape
    ff = wg.shape[-1]

    def kernel(h_ref, wg_ref, wu_ref, wd_ref, o_ref, mid_ref):
        wide = h_ref[...].astype(F32)
        a = normed(wide)
        total = jnp.zeros((TILE, d), F32)
        for lo, hi in pieces(ff, 768):
            gate = jnp.dot(a, wg_ref[:, lo:hi], preferred_element_type=F32)
            up = jnp.dot(a, wu_ref[:, lo:hi], preferred_element_type=F32)
            mid = (gate * jax.nn.sigmoid(gate) * up).astype(BF)
            mid_ref[:, lo:hi] = mid
            total += jnp.dot(mid, wd_ref[lo:hi, :], preferred_element_type=F32)
        o_ref[...] = (wide + total.astype(BF).astype(F32)).astype(BF)

    return pl.pallas_call(
        kernel,
        grid=(tokens // TILE,),
        in_specs=[tiles(d), whole(layer, d, ff), whole(layer, d, ff), whole(layer, ff, d)],
        out_specs=[tiles(d), tiles(ff)],
        out_shape=[jax.ShapeDtypeStruct((tokens, d), BF), jax.ShapeDtypeStruct((tokens, ff), BF)],
        compiler_params=pltpu.CompilerParams(vmem_limit_bytes=LIMIT),
        cost_estimate=pl.CostEstimate(flops=6 * tokens * d * ff, bytes_accessed=2 * 3 * d * ff, transcendentals=tokens * ff),
        name="forward",
    )(h, wg, wu, wd)


def stepped(x, h, mid0, dy, weights, ms, vs, size):
    tokens, d = h.shape
    layers, _, ff = weights[0].shape
    chips, rows = size // 2, d // size
    assert layers == 2 and chips == 4 and ff % d == 0 and ff // size % rows == 0 and d % size == 0
    cuts = ff // d
    blocks = 3 * cuts
    early = 6
    slots = early + cuts
    first = 48
    second = rows - first
    halves = (pl.ds(0, first), pl.ds(first, second))
    parts = 2
    tile = tokens // parts
    small = tile // 2
    per = parts + 2
    lags = (1, 2, 4, 7, 9, 11, 12)
    space = 1
    held = 2
    made = per * cuts
    states_at = made
    again_at = states_at + parts * cuts
    down_at = again_at + held * per
    steps = again_at + cuts + made - 1 + lags[-1]
    assert down_at >= made - 1 + space * (cuts - 1) + lags[-1] and 2 * early >= 2 * cuts and early // 2 * per >= lags[-1]
    MESH = pl.DeviceIdType.MESH

    def kernel(x_ref, h_ref, dy_ref, wg_ref, wu_ref, wd_ref, mid0_hbm, *rest):
        w_hbm, m_hbm, v_hbm = rest[:3], rest[3:6], rest[6:9]
        g_hbm, all_ref, two_hbm = rest[9:12]
        two, a_ref, a_t, dy_all, dy_t, mid, by_g, by_u = rest[12:20]
        own, near, in_a, in_b, gnew, wnew, wold, mold, vold, send, recv, load, keep, away, fetch = rest[20:]
        t = pl.program_id(0)
        me = lax.axis_index("dp")
        chip, core = me // 2, me % 2
        partner = {"dp": me + 1 - 2 * core}

        def at(step):
            return lax.rem(chip + step + chips, chips)

        def dev(step):
            return at(step) * 2 + core

        def slot(q):
            return jnp.where(q < early, q, jnp.where(q < 2 * cuts, q - early, q - 2 * cuts + early))

        def copy(src, dst, kind, q, to):
            n = slot(q)
            return pltpu.make_async_remote_copy(
                src_ref=src, dst_ref=dst, send_sem=send.at[kind, n], recv_sem=recv.at[kind, n], device_id=to, device_id_type=MESH
            )

        def way(q):
            return 1 - 2 * lax.rem(q, 2)

        def over(q):
            return copy(own.at[slot(q), :, 1 - core], near.at[slot(q)], 0, q, partner)

        def message(q, kind, second):
            step = -way(q) if second == (kind != 1) else way(q)
            c = at(2) if kind == 0 else at(step)
            into = in_b if second else in_a
            return copy(own.at[slot(q), c, core, halves[second], :], into.at[slot(q), kind], 1 + 2 * kind + second, q, {"dp": dev(step)})

        def part(q, c, half):
            return own[slot(q), c, core, half, :].astype(F32) + near[slot(q), c, half, :].astype(F32)

        def there(n, q, step):
            return copy(wnew.at[slot(q)], all_ref.at[n, q, me], 7 if step == 1 else 8, q, {"dp": dev(step)})

        def onward(n, q, second):
            step = -way(q) if second else way(q)
            where = all_ref.at[n, q, dev(-step), halves[second], :]
            return copy(where, where, 9 + second, q, {"dp": dev(step)})

        def across(n, q, step):
            where = all_ref.at[n, q, dev(step)]
            return copy(where if step else wnew.at[slot(q)], where, 11 + step + (step < 0) * 4, q, partner)

        def kept(n, q):
            return (
                pltpu.make_async_copy(wnew.at[slot(q)], all_ref.at[n, q, me], keep.at[slot(q), 0]),
                pltpu.make_async_copy(gnew.at[slot(q)], g_hbm.at[n, q], keep.at[slot(q), 1]),
            )

        def loads(n, q, which):
            k = slot(q)
            if which < 2:
                columns = pl.ds(pl.multiple_of(q // 2 * d, 128), d)
                mine, ours = (pl.ds(0, rows), columns), (pl.ds(pl.multiple_of(me * rows, 16), rows), columns)
            else:
                b = jnp.maximum(q - 2 * cuts, 0)
                mine = pl.ds(pl.multiple_of(b * rows, 16), rows), pl.ds(0, d)
                ours = pl.ds(pl.multiple_of(me * (ff // size) + b * rows, 16), rows), pl.ds(0, d)
            return (
                pltpu.make_async_copy(w_hbm[which].at[(n, *ours)], wold.at[k], load.at[k, 0]),
                pltpu.make_async_copy(m_hbm[which].at[(n, *mine)], mold.at[k], load.at[k, 1]),
                pltpu.make_async_copy(v_hbm[which].at[(n, *mine)], vold.at[k], load.at[k, 2]),
            )

        @pl.when(t == 0)
        def _():
            barrier = pltpu.get_barrier_semaphore()
            for to in (partner, {"dp": dev(1)}, {"dp": dev(-1)}):
                pl.semaphore_signal(barrier, inc=1, device_id=to, device_id_type=MESH)
            pl.semaphore_wait(barrier, 3)

        def begin(n, q):
            over(q).start()
            for which, on in enumerate(
                (
                    jnp.logical_and(q < 2 * cuts, lax.rem(q, 2) == 0),
                    jnp.logical_and(q < 2 * cuts, lax.rem(q, 2) == 1),
                    q >= 2 * cuts,
                )
            ):

                @pl.when(on)
                def _(which=which):
                    for one in loads(n, q, which):
                        one.start()

        def split(n, q):
            over(q).wait()
            for kind in (0, 1):
                for second in (0, 1):
                    step = -way(q) if second == (kind != 1) else way(q)
                    c = at(2) if kind == 0 else at(step)
                    own[slot(q), c, core, halves[second], :] = part(q, c, halves[second]).astype(BF)
            for kind in (0, 1):
                for second in (0, 1):
                    message(q, kind, second).start()

        def join(n, q):
            for second, into in ((0, in_a), (1, in_b)):
                message(q, 0, second).wait_recv()
                c = at(-way(q) if second else way(q))
                total = part(q, c, halves[second]) + into[slot(q), 0].astype(F32)
                own[slot(q), c, core, halves[second], :] = total.astype(BF)
            for second in (0, 1):
                message(q, 2, second).start()

        def update(n, q):
            for kind in (1, 2):
                for second in (0, 1):
                    message(q, kind, second).wait_recv()
            for one in loads(n, q, 2):
                one.wait()
            k = slot(q)
            for second, into in ((0, in_a), (1, in_b)):
                half = halves[second]
                g = (part(q, chip, half) + into[k, 1].astype(F32) + into[k, 2].astype(F32)).astype(BF)
                gnew[k, half, :] = g
                wnew[k, half, :] = adamw(wold[k, half, :].astype(F32), mold[k, half, :], vold[k, half, :], g.astype(F32))[0]
            there(n, q, 1).start()
            there(n, q, -1).start()
            across(n, q, 0).start()
            for one in kept(n, q):
                one.start()

        def relay(n, q):
            there(n, q, 1).wait_recv()
            there(n, q, -1).wait_recv()
            onward(n, q, 0).start()
            onward(n, q, 1).start()
            across(n, q, 1).start()
            across(n, q, -1).start()

        def rest_of(n, q):
            onward(n, q, 0).wait_recv()
            onward(n, q, 1).wait_recv()
            across(n, q, 2).start()

        def close(n, q):
            for step in (0, 1, -1, 2):
                across(n, q, step).wait()
            for one in kept(n, q):
                one.wait()
            for kind in range(3):
                for second in (0, 1):
                    message(q, kind, second).wait_send()
            there(n, q, 1).wait_send()
            there(n, q, -1).wait_send()
            onward(n, q, 0).wait_send()
            onward(n, q, 1).wait_send()

        def inside(e, lo, hi):
            return jnp.logical_and(e >= lo, e < hi)

        def again(e):
            return jnp.where(e < down_at, e - again_at, jnp.where(e < down_at + cuts, -1, e - again_at - cuts))

        for lag, act in reversed(tuple(zip(lags, (begin, split, join, update, relay, rest_of, close)))):
            e = t - lag
            n = jnp.where(e < down_at + cuts - 1, 1, 0)
            late = e - jnp.where(n == 1, made - 1, down_at + cuts - 1)
            on = jnp.logical_and(inside(late, 0, cuts * space), lax.rem(late, space) == 0)
            pl.when(on)(functools.partial(act, n, 2 * cuts + late // space))
            n = jnp.where(e < again_at, 1, 0)
            e = jnp.where(n == 1, e, again(e))

            @pl.when(jnp.logical_and(inside(e, 0, made), lax.rem(e, per) == parts))
            def _(act=act, n=n, e=e):
                b = e // per
                act(n, 2 * b)
                act(n, 2 * b + 1)

        last = t < states_at
        i = jnp.where(last, t, again(t))
        b, r = i // per, lax.rem(i, per)
        on = inside(i, 0, made)

        def out_copy(b):
            return pltpu.make_async_copy(two, two_hbm.at[:, :, pl.ds(pl.multiple_of(b * d, 128), d)], away)

        def turn(i):
            j = jnp.where(i < cuts, 0, 1)
            return j, i - j * cuts

        def fetched(i):
            j, k = turn(i)
            n = lax.rem(i, 2)
            return [
                pltpu.make_async_copy(
                    two_hbm.at[which, pl.ds(pl.multiple_of(j * tile, tile), tile), pl.ds(pl.multiple_of(k * d, 128), d)],
                    two.at[n, pl.ds(which * tile, tile)],
                    fetch.at[n, which],
                )
                for which in range(2)
            ]

        def product(i):
            where = mid0_hbm.at[:, pl.ds(pl.multiple_of(i * d, 128), d)]
            return pltpu.make_async_copy(where, two.at[lax.rem(i, 2)], fetch.at[lax.rem(i, 2), 0])

        def spread(g, b):
            for p in range(size):
                n = b * size + p
                owner = n // cuts
                own[early + lax.rem(n, cuts), owner // 2, lax.rem(owner, 2)] = g[p * rows : (p + 1) * rows]

        @pl.when(jnp.logical_and(last, jnp.logical_and(r == 0, b > 0)))
        def _():
            out_copy(b - 1).wait()

        @pl.when(jnp.logical_and(on, r < parts))
        def _():
            def one(piece, _):
                here = pl.ds(pl.multiple_of(r * tile + piece * small, small), small)
                there = pl.ds(pl.multiple_of(piece * small, small), small)

                @pl.when(b == 0)
                def _():
                    @pl.when(last)
                    def _():
                        a_ref[here, :] = normed(h_ref[there, :].astype(F32))
                        dy_all[here, :] = dy_ref[there, :]
                        dy_t[:, here] = dy_ref[there, :].T

                    @pl.when(jnp.logical_not(last))
                    def _():
                        a_ref[here, :] = normed(x_ref[there, :].astype(F32))

                    a_t[:, here] = a_ref[here, :].T

                a = a_ref[here, :]
                gate = jnp.dot(a, wg_ref[...], preferred_element_type=F32)
                up = jnp.dot(a, wu_ref[...], preferred_element_type=F32)
                s = jax.nn.sigmoid(gate)
                silu = gate * s
                mid[here, :] = (silu * up).astype(BF)
                dmid = dot(dy_all[here, :], wd_ref[...], ((1,), (1,))).astype(BF).astype(F32)
                two[0, here, :] = (dmid * up * (s * (1 + gate * (1 - s)))).astype(BF)
                two[1, here, :] = (dmid * silu).astype(BF)
                return 0

            lax.fori_loop(0, 2, one, 0)

            @pl.when(jnp.logical_and(last, r == parts - 1))
            def _():
                out_copy(b).start()

        @pl.when(jnp.logical_and(on, r == parts))
        def _():
            def one(which, _):
                g = jnp.dot(a_t[...], two[which], preferred_element_type=F32).astype(BF)
                own[slot(2 * b + which)] = g.reshape(chips, 2, rows, d)
                return 0

            lax.fori_loop(0, 2, one, 0)

        @pl.when(jnp.logical_and(last, r == per - 1))
        def _():
            spread(jnp.dot(dy_t[...], mid[...], preferred_element_type=F32).astype(BF).T, b)

        @pl.when(t == states_at - 1)
        def _():
            out_copy(cuts - 1).wait()
            for one in fetched(0):
                one.start()

        j = t - states_at

        @pl.when(inside(j, 0, parts * cuts))
        def _():
            which, k = turn(j)
            for one in fetched(j):
                one.wait()

            @pl.when(j < parts * cuts - 1)
            def _():
                for one in fetched(j + 1):
                    one.start()

            @pl.when(k == 0)
            def _():
                by_g[...] = jnp.zeros_like(by_g)
                by_u[...] = jnp.zeros_like(by_u)

            for piece in range(2):
                there = pl.ds(piece * small, small)
                by_g[there, :] += dot(two[lax.rem(j, 2), there, :], wg_ref[...], ((1,), (1,)))
                by_u[there, :] += dot(two[lax.rem(j, 2), pl.ds(tile + piece * small, small), :], wu_ref[...], ((1,), (1,)))

            @pl.when(k == cuts - 1)
            def _():
                for piece in range(2):
                    here = pl.ds(pl.multiple_of(which * tile + piece * small, small), small)
                    there = pl.ds(piece * small, small)
                    da = (by_g[there, :].astype(BF).astype(F32) + by_u[there, :].astype(BF).astype(F32)).astype(BF).astype(F32)
                    wide = h_ref[there, :].astype(F32)
                    scale = lax.rsqrt(jnp.mean(wide * wide, -1, keepdims=True) + 1e-6)
                    inner = jnp.mean(da * wide, -1, keepdims=True)
                    back = (da * scale - wide * (inner * scale * scale * scale)).astype(BF)
                    new = (dy_all[here, :].astype(F32) + back.astype(F32)).astype(BF)
                    dy_all[here, :] = new
                    dy_t[:, here] = new.T

        @pl.when(t == down_at - 1)
        def _():
            product(0).start()

        @pl.when(inside(t, down_at, down_at + cuts))
        def _():
            k = t - down_at
            product(k).wait()

            @pl.when(k < cuts - 1)
            def _():
                product(k + 1).start()

            spread(jnp.dot(dy_t[...], two[lax.rem(k, 2)], preferred_element_type=F32).astype(BF).T, k)

    def block(t):
        again = jnp.where(t < down_at, t - again_at, jnp.maximum(t - again_at - cuts, held * per - 1))
        again = jnp.clip(jnp.maximum(again, 0) // per, 0, cuts - 1)
        b = jnp.where(t < states_at, t // per, jnp.where(t < again_at, lax.rem(jnp.maximum(t - states_at, 0), cuts), again))
        return jnp.where(t < again_at, 1, 0), b

    def at_states(t):
        return jnp.where(t < states_at, jnp.minimum(t, parts - 1), jnp.where(t < states_at + cuts, 0, 1)), 0

    wide = pl.BlockSpec((None, d, d), lambda t: (block(t)[0], 0, block(t)[1]))
    tall = pl.BlockSpec((None, d, d), lambda t: (*block(t), 0))
    hbm = pl.BlockSpec(memory_space=pl.ANY)
    return pl.pallas_call(
        kernel,
        grid=(steps,),
        in_specs=[
            pl.BlockSpec((tile, d), lambda t: (jnp.clip(t - again_at, 0, parts - 1), 0), pipeline_mode=pl.Buffered(1)),
            pl.BlockSpec((tile, d), at_states, pipeline_mode=pl.Buffered(1)),
            pl.BlockSpec((tile, d), lambda t: (jnp.minimum(t, parts - 1), 0), pipeline_mode=pl.Buffered(1)),
            wide,
            wide,
            tall,
        ]
        + [hbm] * 10,
        out_specs=[hbm] * 3,
        out_shape=[
            jax.ShapeDtypeStruct((layers, blocks, rows, d), BF),
            jax.ShapeDtypeStruct((layers, blocks, size, rows, d), BF),
            jax.ShapeDtypeStruct((2, tokens, ff), BF),
        ],
        scratch_shapes=[
            pltpu.VMEM((2, tokens, d), BF),
            pltpu.VMEM((tokens, d), BF),
            pltpu.VMEM((d, tokens), BF),
            pltpu.VMEM((tokens, d), BF),
            pltpu.VMEM((d, tokens), BF),
            pltpu.VMEM((tokens, d), BF),
            pltpu.VMEM((tile, d), F32),
            pltpu.VMEM((tile, d), F32),
            pltpu.VMEM((slots, chips, 2, rows, d), BF),
            pltpu.VMEM((slots, chips, rows, d), BF),
            pltpu.VMEM((slots, 3, first, d), BF),
            pltpu.VMEM((slots, 3, second, d), BF),
            pltpu.VMEM((slots, rows, d), BF),
            pltpu.VMEM((slots, rows, d), BF),
            pltpu.VMEM((slots, rows, d), BF),
            pltpu.VMEM((slots, rows, d), F32),
            pltpu.VMEM((slots, rows, d), F32),
            pltpu.SemaphoreType.DMA((15, slots)),
            pltpu.SemaphoreType.DMA((15, slots)),
            pltpu.SemaphoreType.DMA((slots, 3)),
            pltpu.SemaphoreType.DMA((slots, 2)),
            pltpu.SemaphoreType.DMA,
            pltpu.SemaphoreType.DMA((2, 2)),
        ],
        compiler_params=pltpu.CompilerParams(vmem_limit_bytes=LIMIT, collective_id=0, has_side_effects=True),
        cost_estimate=pl.CostEstimate(flops=26 * tokens * d * ff, bytes_accessed=4 * 3 * tokens * ff, transcendentals=0),
        name="stepped",
    )(x, h, dy, *weights, mid0, *weights, *ms, *vs)


def assembled(gathered):
    layers, blocks, size, rows, d = gathered.shape
    cuts = blocks // 3
    ff = cuts * d

    def kernel(ref, g_ref, u_ref, d_ref):
        for p in range(2):
            for b in range(cuts):
                g_ref[p * rows : (p + 1) * rows, b * d : (b + 1) * d] = ref[2 * b, p]
                u_ref[p * rows : (p + 1) * rows, b * d : (b + 1) * d] = ref[2 * b + 1, p]
                d_ref[(p * cuts + b) * rows : (p * cuts + b + 1) * rows, :] = ref[2 * cuts + b, p]

    wide = pl.BlockSpec((None, 2 * rows, ff), lambda n, p: (n, p, 0))
    tall = pl.BlockSpec((None, 2 * ff // size, d), lambda n, p: (n, p, 0))
    return pl.pallas_call(
        kernel,
        grid=(layers, size // 2),
        in_specs=[pl.BlockSpec((None, blocks, 2, rows, d), lambda n, p: (n, 0, p, 0, 0))],
        out_specs=[wide, wide, tall],
        out_shape=[jax.ShapeDtypeStruct((layers, d, ff), BF)] * 2 + [jax.ShapeDtypeStruct((layers, ff, d), BF)],
        name="assembled",
    )(gathered)


def moments(sums, ms, vs):
    layers, blocks, rows, d = sums.shape
    cuts = blocks // 3

    def kernel(g_ref, *refs):
        b = pl.program_id(1)
        for i, q in enumerate((2 * b, 2 * b + 1, 2 * cuts + b)):
            g = g_ref[q].astype(F32)
            _, refs[6 + i][...], refs[9 + i][...] = adamw(jnp.zeros_like(g), refs[i][...], refs[3 + i][...], g)

    wide = pl.BlockSpec((None, rows, d), lambda n, b: (n, 0, b))
    tall = pl.BlockSpec((None, rows, d), lambda n, b: (n, b, 0))
    return pl.pallas_call(
        kernel,
        grid=(layers, cuts),
        in_specs=[pl.BlockSpec((None, blocks, rows, d), lambda n, b: (n, 0, 0, 0))] + [wide, wide, tall] * 2,
        out_specs=[wide, wide, tall] * 2,
        out_shape=[jax.ShapeDtypeStruct(t.shape, F32) for t in ms] * 2,
        name="moments",
    )(sums, *ms, *vs)


def solution(mesh):
    size = mesh.shape["dp"]

    def body(x, dy, *arrays):
        weights, ms, vs = (arrays[i : i + 3] for i in (0, 3, 6))
        h, mid0 = forward(x[0], *weights, 0)
        sums, gathered, _ = stepped(x[0], h, mid0, dy[0], weights, ms, vs, size)
        return (*assembled(gathered), *moments(sums, ms, vs))

    rows = P(None, "dp", None)
    seqs = P(("rep", "dp"), None, None)
    return jax.shard_map(
        body,
        mesh=mesh,
        in_specs=(seqs, seqs, P(), P(), P()) + (rows,) * 6,
        out_specs=(P("rep", None, None),) * 3 + (P("rep", "dp", None),) * 6,
        check_vma=False,
    )
```
